32 devices in a mesh: ga: 8 (over y, x, core), ba: 4 (over z).
Axes of the slice: x: 2, y: 2, z: 4, core: 2. Of those that a mesh axis runs over, the one named last changes fastest.
Arguments:
- psi: float32 [2, 16384, 2048], P(None, 'ga', 'ba'), may hold values from -0.1875 to 0.1875
- dpsi: float32 [2, 16384, 512], P(None, 'ga', 'ba'), may hold values from -6 to 6
- band_weight: float32 [2048], replicated, may hold values from 0.25 to 1
- panel_band: int32 [16], P('ba'), may hold values from 0 to 15, each once
- slab_offset: int32 [8], replicated, may hold values from 0 to 2047
Outputs:
- projected: float32 [2, 16384, 512], P(None, 'ga', 'ba')
The draws below stay inside these ranges and needn't reach their ends.
Inputs may be any that keep to these rules, and one draw needn't show every extreme that they name: panel_band is a permutation of the panel numbers.
All inputs are finite; a program needn't handle non-finite values.
Results may differ from the reference program's by a relative error of at most 0.00012.
Values sent between devices are 32-bit elements; how exact they have to be, the bound alone decides.
A program may use at most 128 MiB of HBM per device.

```python
import math
import jax
import jax.numpy as jnp
from jax import lax

NB = 2048
NP = 512
PANEL = 128
NPW_DEV = 2048
NPW = 16384
NPANEL = 16
N_GA = 8


def place_ends(array, rng, low, high):
    place = [jax.random.randint(jax.random.fold_in(rng, axis), (), 0, length) for axis, length in enumerate(array.shape)]
    widest = array.shape.index(max(array.shape))
    neighbour = place[:widest] + [(place[widest] + 1) % array.shape[widest]] + place[widest + 1:]
    return array.at[tuple(place)].set(low).at[tuple(neighbour)].set(high)


def block_scale(rng, shape, shards, least, top_value):
    def one(position, shards_of):
        steps = jax.random.uniform(jax.random.fold_in(jax.random.fold_in(rng, 6), position), (shards_of,), jnp.float32, least / len(shards), top_value / len(shards))
        return jnp.repeat(jnp.exp(steps), shape[position] // shards_of).reshape((-1,) + (1,) * (len(shape) - position - 1))

    factor_of = one(*shards[0])
    for cut in shards[1:]:
        factor_of = factor_of * one(*cut)
    return factor_of


def scatter_about(key, extent, deviation, reach, shards=(), held_as=jnp.bfloat16):
    drawn = jax.random.normal(key, extent, jnp.float32) * deviation
    if len(shards) > 0:
        drawn = block_scale(key, extent, shards, -0.22, 0.18) * drawn
    return jnp.clip(drawn, min=-reach, max=reach).astype(held_as)


def setup_inputs(seed: int = 0) -> dict:
    seeds = jax.random.split(jax.random.key(seed), 6)
    return {
        "psi": scatter_about(seeds[0], (2, NPW, NB), ((NPW * NB) ** -0.25), 0.1875, ((1, 8), (2, 4)), jnp.float32),
        "dpsi": scatter_about(seeds[1], (2, NPW, NP), 1.0, 6.0, ((1, 8), (2, 4)), jnp.float32),
        "band_weight": jnp.clip(jnp.exp(jax.random.uniform(seeds[2], (NB,), jnp.float32, math.log(0.25), math.log(1.0))), 0.25, 1.0),
        "panel_band": jax.random.permutation(seeds[3], NPANEL).astype(jnp.int32),
        "slab_offset": place_ends(jax.random.randint(seeds[4], (N_GA,), 0, NPW_DEV), jax.random.fold_in(seeds[4], 1), 0, NPW_DEV - 1).astype(jnp.int32),
    }


def tdot(left, right):
    return lax.dot_general(left, right, (((0,), (0,)), ((), ())), precision=lax.Precision.HIGHEST, preferred_element_type=jnp.float32)


def mdot(left, right):
    return jnp.dot(left, right, precision=lax.Precision.HIGHEST, preferred_element_type=jnp.float32)


def reference(psi, dpsi, band_weight, panel_band, slab_offset):
    stacked = dpsi.reshape(2, N_GA, NPW_DEV, NP)
    rows = (jnp.arange(NPW_DEV, dtype=jnp.int32)[None, :] + slab_offset[:, None]) % NPW_DEV
    aligned = jnp.take_along_axis(stacked, rows[None, :, :, None], axis=2).reshape(2, NPW, NP)
    weight = band_weight.reshape(NPANEL, PANEL)[panel_band].reshape(NB)
    over_re = tdot(psi[0], aligned[0]) + tdot(psi[1], aligned[1])
    over_im = tdot(psi[0], aligned[1]) - tdot(psi[1], aligned[0])
    w_re = over_re * weight[:, None]
    w_im = over_im * weight[:, None]
    corr_re = mdot(psi[0], w_re) - mdot(psi[1], w_im)
    corr_im = mdot(psi[0], w_im) + mdot(psi[1], w_re)
    diff = (aligned - jnp.stack([corr_re, corr_im])).reshape(2, N_GA, NPW_DEV, NP)
    back = (jnp.arange(NPW_DEV, dtype=jnp.int32)[None, :] - slab_offset[:, None]) % NPW_DEV
    result = jnp.take_along_axis(diff, back[None, :, :, None], axis=2)
    return result.reshape(2, NPW, NP)
```

```python
import functools

import jax
import jax.numpy as jnp
from jax import lax
from jax.experimental import pallas as pl
from jax.experimental.pallas import tpu as pltpu
from jax.sharding import PartitionSpec as P

MESH = pl.DeviceIdType.MESH
LANES = 128
HALF = LANES // 2
PIECES = 4
TILE = 256
BF16 = jnp.bfloat16
F32 = jnp.float32


def split(value):
    high = value.astype(BF16)
    return high, (value - high.astype(F32)).astype(BF16)


def turned(packed):
    lane = lax.broadcasted_iota(jnp.int32, packed.shape, 1)
    other = pltpu.roll(packed, HALF, axis=1)
    return jnp.where(lane < HALF, other, -other)


def pdot(left, right):
    return jnp.dot(left, right, preferred_element_type=F32)


def kernel(
    G, B, U, K, delay,
    offset_ref, panel_ref, weight_ref, psi_ref, dpsi_ref, out_ref,
    psi_t, psi_w, a_ref, s_ref, c_ref, parts, r_ref, m_ref, acc, x_ref,
    psi_sem, a_send, a_recv, s_send, s_recv, m_send, m_recv,
):
    rows, cols = dpsi_ref.shape[1:]
    nb = psi_ref.shape[2]
    tiles = nb // LANES
    pr = rows // PIECES
    nr = nb // G
    g = lax.axis_index("ga")
    z = lax.axis_index("ba")

    def psi_copies():
        for part in range(2):
            for t in range(tiles):
                i = part * tiles + t
                lanes = pl.ds(t * LANES, LANES)
                yield pltpu.make_async_copy(
                    psi_ref.at[part, :, lanes], c_ref.at[i, pl.ds(0, rows)], psi_sem.at[0, i]
                )
                yield pltpu.make_async_copy(
                    psi_ref.at[part, pl.ds(0, TILE), lanes],
                    c_ref.at[i, pl.ds(rows, TILE)],
                    psi_sem.at[1, i],
                )

    for copy in psi_copies():
        copy.start()

    barrier = pltpu.get_barrier_semaphore()
    for q in range(1, G):
        pl.semaphore_signal(barrier, inc=1, device_id={"ga": lax.rem(g + q, G)}, device_id_type=MESH)

    @pl.when(z > 0)
    def _():
        pl.semaphore_signal(barrier, inc=1, device_id={"ba": z - 1}, device_id_type=MESH)

    @pl.when(z < B - 1)
    def _():
        pl.semaphore_signal(barrier, inc=1, device_id={"ba": z + 1}, device_id_type=MESH)

    pl.semaphore_wait(barrier, G - 1 + jnp.where(z > 0, 1, 0) + jnp.where(z < B - 1, 1, 0))

    def place(lane):
        return z if lane == 0 else B - 1 - z

    def true(lane, index):
        return index if lane == 0 else B - 1 - index

    def piece(p):
        return pl.ds(pl.multiple_of(p * pr, pr), pr)

    def a_copy(lane, unit, p):
        return pltpu.make_async_remote_copy(
            a_ref.at[unit, piece(p)], a_ref.at[unit, piece(p)],
            a_send.at[lane, unit, p], a_recv.at[unit, p],
            device_id={"ba": true(lane, jnp.minimum(place(lane) + 1, B - 1))}, device_id_type=MESH,
        )

    def s_slot(lane, at, dest, u):
        shared = true(lane, dest) * U + u
        if lane == 0:
            return shared
        return jnp.where(dest == at, B * U + u, shared)

    def s_copy(lane, source, unit, slot, p):
        return pltpu.make_async_remote_copy(
            source, s_ref.at[slot, piece(p)], s_send.at[unit, p], s_recv.at[slot, p],
            device_id={"ba": true(lane, jnp.minimum(place(lane) + 1, B - 1))}, device_id_type=MESH,
        )

    def s_wait(slot, p):
        ref = s_ref.at[slot, piece(p)]
        pltpu.make_async_copy(ref, ref, s_recv.at[slot, p]).wait()

    def gathered(lane, k):
        at = place(lane)
        count = U * at
        arrives = (k >= 1) & (k <= count)
        if U == 2:
            index = jnp.where(k <= at, at - k, k - at - 1)
            u = jnp.where(k <= at, 0, 1)
        else:
            index, u = at - k, 0 * k
        own = (2 * at + lane < B) & (k > count) & (k <= count + U)
        index = jnp.where(own, at, index)
        u = jnp.where(own, k - count - 1, u)
        has = arrives | own
        unit = jnp.where(has, true(lane, index) * U + u, 0)
        return arrives, has, unit

    def reduced(lane, k):
        at = place(lane)
        m = k - U * at - delay
        arrives = (at > 0) & (m >= 1) & (m <= U * (B - at))
        if U == 2:
            dest = jnp.where(m <= B - at, at + m - 1, 2 * B - at - m)
            u = jnp.where(m <= B - at, 0, 1)
        else:
            dest, u = at + m - 1, 0 * k
        dest = jnp.where(arrives, dest, at)
        return arrives, dest, u

    for u in range(U):
        for p in range(PIECES):
            span = pl.ds(p * pr, pr)
            own = slice(u * HALF, (u + 1) * HALF)
            a_ref[z * U + u, span, :] = jnp.concatenate(
                [dpsi_ref[0, span, own], dpsi_ref[1, span, own]], axis=1
            )
            if u == 0:
                for lane in range(2):
                    @pl.when(place(lane) < B - 1)
                    def _(lane=lane, p=p):
                        a_copy(lane, z * U, p).start()

    def send_last(lane):
        if U == 2:
            for p in range(PIECES):
                a_copy(lane, z * U + 1, p).start()

    for lane in range(2):
        @pl.when((place(lane) == 0) & (B > 1))
        def _(lane=lane):
            send_last(lane)

    for copy in psi_copies():
        copy.wait()
    offset = offset_ref[g]
    for part in range(2):
        for t in range(tiles):
            i = part * tiles + t
            row = weight_ref[pl.ds(panel_ref[t], 1), :]

            def load(n, carry, i=i, row=row):
                start = lax.rem(n * TILE - offset + rows, rows)
                block = c_ref[i, pl.ds(start, TILE), :]
                span = pl.ds(pl.multiple_of(n * TILE, TILE), TILE)
                bands = slice(i * LANES, (i + 1) * LANES)
                high, rest = split(block.T)
                psi_t[0, bands, span] = high
                psi_t[1, bands, span] = rest
                high, rest = split(block * row)
                psi_w[0, span, bands] = high
                psi_w[1, span, bands] = rest
                return carry

            lax.fori_loop(0, rows // TILE, load, 0)

    def margin(lane, unit, p):
        high, rest = split(a_ref[unit, piece(p), :])
        right = jnp.concatenate([high, rest], axis=1)
        for block in range(0, 2 * nb, TILE):
            bands = slice(block, block + TILE)
            wide = pdot(psi_t[0, bands, piece(p)], right) + pdot(psi_t[1, bands, piece(p)], right)
            narrow = wide[:, :LANES] + wide[:, LANES:]
            acc[lane, bands, :] = jnp.where(p == 0, 0.0, acc[lane, bands, :]) + narrow

    def exchange(lane, unit, phase, start):
        for q in range(1, G):
            peer = lax.rem(g + q, G)
            if phase == 0:
                source = parts.at[lane, pl.ds(pl.multiple_of(peer * nr, nr), nr)]
                target = r_ref.at[unit, q - 1]
            else:
                source = m_ref.at[unit, pl.ds(pl.multiple_of(g * nr, nr), nr)]
                target = source
            pltpu.make_async_remote_copy(
                source, target, m_send.at[phase, unit], m_recv.at[phase, unit],
                device_id={"ga": peer}, device_id_type=MESH,
            ).start()

    def exchange_wait(unit, sem):
        ref = r_ref.at[unit]
        pltpu.make_async_copy(ref, ref, sem).wait()

    def publish(lane, unit):
        parts[lane] = acc[lane, :nb, :] + turned(acc[lane, nb:, :])
        exchange(lane, unit, 0, True)

    def reduce(lane, unit):
        exchange_wait(unit, m_recv.at[0, unit])
        exchange_wait(unit, m_send.at[0, unit])
        mine = pl.ds(pl.multiple_of(g * nr, nr), nr)
        total = parts[lane, mine, :]
        for q in range(1, G):
            total = total + r_ref[unit, q - 1]
        m_ref[unit, mine, :] = total
        exchange(lane, unit, 1, True)

    def collect(lane, unit):
        exchange_wait(unit, m_recv.at[1, unit])
        whole = m_ref[unit]
        high, rest = split(whole)
        x_ref[lane, :nb, :LANES] = high
        x_ref[lane, :nb, LANES:] = rest
        high, rest = split(-turned(whole))
        x_ref[lane, nb:, :LANES] = high
        x_ref[lane, nb:, LANES:] = rest

    def correct(lane, unit, p):
        right = x_ref[lane]
        for block in range(0, pr, TILE):
            span = pl.ds(pl.multiple_of(p * pr + block, TILE), TILE)
            wide = pdot(psi_w[0, span, :], right) + pdot(psi_w[1, span, :], right)
            c_ref[unit, span, :] = wide[:, :LANES] + wide[:, LANES:]

    def step(n, carry):
        k, p = n // PIECES + 1, lax.rem(n, PIECES)
        for lane in range(2):
            at = place(lane)
            arrives, has, unit = gathered(lane, k)

            @pl.when(arrives)
            def _(lane=lane, at=at, unit=unit):
                a_copy(lane, unit, p).wait_recv()

                @pl.when(at < B - 1)
                def _():
                    a_copy(lane, unit, p).start()

            if U == 2:
                @pl.when((at > 0) & (at < B - 1) & (k == U * at) & (p == PIECES - 1))
                def _(lane=lane):
                    send_last(lane)

            arrives, dest, u = reduced(lane, k)

            @pl.when(arrives)
            def _(lane=lane, at=at, dest=dest, u=u):
                slot = s_slot(lane, at, dest, u)
                s_wait(slot, p)

                @pl.when(dest > at)
                def _():
                    unit = true(lane, dest) * U + u
                    s_ref[slot, piece(p), :] = s_ref[slot, piece(p), :] + c_ref[unit, piece(p), :]
                    s_copy(lane, s_ref.at[slot, piece(p)], unit, s_slot(lane, at + 1, dest, u), p).start()

        for lane in range(2):
            _, has, unit = gathered(lane, k - 1)

            @pl.when(has & (p == 0))
            def _(lane=lane, unit=unit):
                reduce(lane, unit)

            @pl.when(has & (p == 1))
            def _(lane=lane, unit=unit):
                collect(lane, unit)

            @pl.when(has & ((p == 1) | (p == 2)))
            def _(lane=lane, unit=unit):
                away = 1 - lane

                def one(i, carry):
                    c = 2 * (p - 1) + i
                    correct(lane, unit, c)

                    @pl.when((place(away) == 0) & (unit // U != z))
                    def _():
                        dest = true(away, unit // U)
                        slot = s_slot(away, 1, dest, lax.rem(unit, U))
                        s_copy(away, c_ref.at[unit, piece(c)], unit, slot, c).start()

                    return carry

                lax.fori_loop(0, PIECES // 2, one, 0)

        for lane in range(2):
            _, has, unit = gathered(lane, k)

            @pl.when(has)
            def _(lane=lane, unit=unit):
                margin(lane, unit, p)

                @pl.when(p == PIECES - 1)
                def _():
                    publish(lane, unit)

        return carry

    lax.fori_loop(0, K * PIECES, step, 0)

    def finish(p, carry):
        sums = []
        for u in range(U):
            unit = z * U + u
            total = c_ref[unit, piece(p), :]
            total = total + jnp.where(z > 0, s_ref[unit, piece(p), :], 0.0)
            total = total + jnp.where(z < B - 1, s_ref[B * U + u, piece(p), :], 0.0)
            sums.append(a_ref[unit, piece(p), :] - total)
        for part in range(2):
            half = slice(part * HALF, (part + 1) * HALF)
            out_ref[part, piece(p), :] = jnp.concatenate([total[:, half] for total in sums], axis=1)
        return carry

    lax.fori_loop(0, PIECES, finish, 0)

    def drain(n, carry):
        unit, p = n // PIECES, lax.rem(n, PIECES)
        block = unit // U

        @pl.when((block <= z) & (z < B - 1))
        def _():
            a_copy(0, unit, p).wait_send()

        @pl.when((block >= z) & (z > 0))
        def _():
            a_copy(1, unit, p).wait_send()

        @pl.when(block != z)
        def _():
            ref = s_ref.at[unit, piece(p)]
            pltpu.make_async_copy(ref, ref, s_send.at[unit, p]).wait()

        @pl.when(p == 0)
        def _():
            exchange_wait(unit, m_send.at[1, unit])

        return carry

    lax.fori_loop(0, B * U * PIECES, drain, 0)


def per_device(G, B, psi, dpsi, band_weight, panel_band, slab_offset):
    _, rows, cols = dpsi.shape
    nb = psi.shape[2]
    U = cols // HALF
    delay = 2 - U
    K = U * B + delay
    units = B * U
    weight = band_weight.reshape(-1, LANES)
    smem = pl.BlockSpec(memory_space=pltpu.SMEM)
    vmem = pl.BlockSpec(memory_space=pltpu.VMEM)
    flops = 2 * 2 * 2 * (2 * nb) * rows * (2 * LANES) * units
    return pl.pallas_call(
        functools.partial(kernel, G, B, U, K, delay),
        out_shape=jax.ShapeDtypeStruct(dpsi.shape, F32),
        in_specs=[smem, smem, vmem, pl.BlockSpec(memory_space=pl.ANY), vmem],
        out_specs=vmem,
        scratch_shapes=[
            pltpu.VMEM((2, 2 * nb, rows), BF16),
            pltpu.VMEM((2, rows, 2 * nb), BF16),
            pltpu.VMEM((units, rows, LANES), F32),
            pltpu.VMEM((units + U, rows, LANES), F32),
            pltpu.VMEM((max(units, 2 * nb // LANES), rows + TILE, LANES), F32),
            pltpu.VMEM((2, nb, LANES), F32),
            pltpu.VMEM((units, G - 1, nb // G, LANES), F32),
            pltpu.VMEM((units, nb, LANES), F32),
            pltpu.VMEM((2, 2 * nb, LANES), F32),
            pltpu.VMEM((2, 2 * nb, 2 * LANES), BF16),
            pltpu.SemaphoreType.DMA((2, 2 * nb // LANES)),
            pltpu.SemaphoreType.DMA((2, units, PIECES)),
            pltpu.SemaphoreType.DMA((units, PIECES)),
            pltpu.SemaphoreType.DMA((units, PIECES)),
            pltpu.SemaphoreType.DMA((units + U, PIECES)),
            pltpu.SemaphoreType.DMA((2, units)),
            pltpu.SemaphoreType.DMA((2, units)),
        ],
        compiler_params=pltpu.CompilerParams(
            collective_id=0, has_side_effects=True, vmem_limit_bytes=67043328
        ),
        cost_estimate=pl.CostEstimate(flops=flops, bytes_accessed=12 << 20, transcendentals=0),
        name="project",
    )(slab_offset, panel_band, weight, psi, dpsi)


def solution(mesh):
    in_specs = (P(None, "ga", "ba"), P(None, "ga", "ba"), P(), P("ba"), P())
    out_specs = P(None, "ga", "ba")
    return jax.shard_map(
        functools.partial(per_device, mesh.shape["ga"], mesh.shape["ba"]),
        mesh=mesh, in_specs=in_specs, out_specs=out_specs, check_vma=False,
    )
```

```python
import functools

import jax
import jax.numpy as jnp
from jax import lax
from jax.experimental import pallas as pl
from jax.experimental.pallas import tpu as pltpu
from jax.sharding import PartitionSpec as P

MESH = pl.DeviceIdType.MESH
LANES = 128
HALF = LANES // 2
PIECES = 4
TILE = 256
BF16 = jnp.bfloat16
F32 = jnp.float32


def split(value):
    high = value.astype(BF16)
    return high, (value - high.astype(F32)).astype(BF16)


def turned(packed):
    lane = lax.broadcasted_iota(jnp.int32, packed.shape, 1)
    other = pltpu.roll(packed, HALF, axis=1)
    return jnp.where(lane < HALF, other, -other)


def pdot(left, right):
    return jnp.dot(left, right, preferred_element_type=F32)


def kernel(
    G, B, U, K, delay,
    offset_ref, panel_ref, weight_ref, psi_ref, dpsi_ref, out_ref,
    psi_t, psi_w, a_ref, s_ref, c_ref, parts, r_ref, m_ref, acc, x_ref,
    psi_sem, dpsi_sem, a_send, a_recv, s_send, s_recv, m_send, m_recv,
):
    rows, cols = dpsi_ref.shape[1:]
    nb = psi_ref.shape[2]
    tiles = nb // LANES
    pr = rows // PIECES
    nr = nb // G
    g = lax.axis_index("ga")
    z = lax.axis_index("ba")

    def psi_copies():
        for part in range(2):
            for t in range(tiles):
                i = part * tiles + t
                lanes = pl.ds(t * LANES, LANES)
                yield pltpu.make_async_copy(
                    psi_ref.at[part, :, lanes], c_ref.at[i, pl.ds(0, rows)], psi_sem.at[0, i]
                )
                yield pltpu.make_async_copy(
                    psi_ref.at[part, pl.ds(0, TILE), lanes],
                    c_ref.at[i, pl.ds(rows, TILE)],
                    psi_sem.at[1, i],
                )

    def dpsi_copy(p):
        span = pl.ds(p * pr, pr)
        return pltpu.make_async_copy(dpsi_ref.at[:, span], out_ref.at[:, span], dpsi_sem.at[p])

    for p in range(PIECES):
        dpsi_copy(p).start()
    for copy in psi_copies():
        copy.start()

    barrier = pltpu.get_barrier_semaphore()
    for q in range(1, G):
        pl.semaphore_signal(barrier, inc=1, device_id={"ga": lax.rem(g + q, G)}, device_id_type=MESH)

    @pl.when(z > 0)
    def _():
        pl.semaphore_signal(barrier, inc=1, device_id={"ba": z - 1}, device_id_type=MESH)

    @pl.when(z < B - 1)
    def _():
        pl.semaphore_signal(barrier, inc=1, device_id={"ba": z + 1}, device_id_type=MESH)

    pl.semaphore_wait(barrier, G - 1 + jnp.where(z > 0, 1, 0) + jnp.where(z < B - 1, 1, 0))

    def place(lane):
        return z if lane == 0 else B - 1 - z

    def true(lane, index):
        return index if lane == 0 else B - 1 - index

    def piece(p):
        return pl.ds(pl.multiple_of(p * pr, pr), pr)

    def a_copy(lane, unit, p):
        return pltpu.make_async_remote_copy(
            a_ref.at[unit, piece(p)], a_ref.at[unit, piece(p)],
            a_send.at[lane, unit, p], a_recv.at[unit, p],
            device_id={"ba": true(lane, jnp.minimum(place(lane) + 1, B - 1))}, device_id_type=MESH,
        )

    def s_slot(lane, at, dest, u):
        shared = true(lane, dest) * U + u
        if lane == 0:
            return shared
        return jnp.where(dest == at, B * U + u, shared)

    def s_copy(lane, source, unit, slot, p):
        return pltpu.make_async_remote_copy(
            source, s_ref.at[slot, piece(p)], s_send.at[unit, p], s_recv.at[slot, p],
            device_id={"ba": true(lane, jnp.minimum(place(lane) + 1, B - 1))}, device_id_type=MESH,
        )

    def s_wait(slot, p):
        ref = s_ref.at[slot, piece(p)]
        pltpu.make_async_copy(ref, ref, s_recv.at[slot, p]).wait()

    def gathered(lane, k):
        at = place(lane)
        count = U * at
        arrives = (k >= 1) & (k <= count)
        if U == 2:
            index = jnp.where(k <= at, at - k, k - at - 1)
            u = jnp.where(k <= at, 0, 1)
        else:
            index, u = at - k, 0 * k
        own = (2 * at + lane < B) & (k > count) & (k <= count + U)
        index = jnp.where(own, at, index)
        u = jnp.where(own, k - count - 1, u)
        has = arrives | own
        unit = jnp.where(has, true(lane, index) * U + u, 0)
        return arrives, has, unit

    def reduced(lane, k):
        at = place(lane)
        m = k - U * at - delay
        arrives = (at > 0) & (m >= 1) & (m <= U * (B - at))
        if U == 2:
            dest = jnp.where(m <= B - at, at + m - 1, 2 * B - at - m)
            u = jnp.where(m <= B - at, 0, 1)
        else:
            dest, u = at + m - 1, 0 * k
        dest = jnp.where(arrives, dest, at)
        return arrives, dest, u

    def pack(u, p):
        span = pl.ds(p * pr, pr)
        own = slice(u * HALF, (u + 1) * HALF)
        a_ref[z * U + u, span, :] = jnp.concatenate(
            [out_ref[0, span, own], out_ref[1, span, own]], axis=1
        )

    for p in range(PIECES):
        dpsi_copy(p).wait()
        pack(0, p)
        for lane in range(2):
            @pl.when(place(lane) < B - 1)
            def _(lane=lane, p=p):
                a_copy(lane, z * U, p).start()
    for u in range(1, U):
        for p in range(PIECES):
            pack(u, p)

    def send_last(lane):
        if U == 2:
            for p in range(PIECES):
                a_copy(lane, z * U + 1, p).start()

    for lane in range(2):
        @pl.when((place(lane) == 0) & (B > 1))
        def _(lane=lane):
            send_last(lane)

    for copy in psi_copies():
        copy.wait()
    offset = offset_ref[g]
    for part in range(2):
        for t in range(tiles):
            i = part * tiles + t
            row = weight_ref[pl.ds(panel_ref[t], 1), :]

            def load(n, carry, i=i, row=row):
                start = lax.rem(n * TILE - offset + rows, rows)
                block = c_ref[i, pl.ds(start, TILE), :]
                span = pl.ds(pl.multiple_of(n * TILE, TILE), TILE)
                bands = slice(i * LANES, (i + 1) * LANES)
                high, rest = split(block.T)
                psi_t[0, bands, span] = high
                psi_t[1, bands, span] = rest
                high, rest = split(block * row)
                psi_w[0, span, bands] = high
                psi_w[1, span, bands] = rest
                return carry

            lax.fori_loop(0, rows // TILE, load, 0)

    def margin(lane, unit, p):
        high, rest = split(a_ref[unit, piece(p), :])
        right = jnp.concatenate([high, rest], axis=1)
        for block in range(0, 2 * nb, TILE):
            bands = slice(block, block + TILE)
            wide = pdot(psi_t[0, bands, piece(p)], right) + pdot(psi_t[1, bands, piece(p)], right)
            narrow = wide[:, :LANES] + wide[:, LANES:]
            acc[lane, bands, :] = jnp.where(p == 0, 0.0, acc[lane, bands, :]) + narrow

    def exchange(lane, unit, phase, start):
        for q in range(1, G):
            peer = lax.rem(g + q, G)
            if phase == 0:
                source = parts.at[lane, pl.ds(pl.multiple_of(peer * nr, nr), nr)]
                target = r_ref.at[unit, q - 1]
            else:
                source = m_ref.at[unit, pl.ds(pl.multiple_of(g * nr, nr), nr)]
                target = source
            pltpu.make_async_remote_copy(
                source, target, m_send.at[phase, unit], m_recv.at[phase, unit],
                device_id={"ga": peer}, device_id_type=MESH,
            ).start()

    def exchange_wait(unit, sem):
        ref = r_ref.at[unit]
        pltpu.make_async_copy(ref, ref, sem).wait()

    def publish(lane, unit):
        parts[lane] = acc[lane, :nb, :] + turned(acc[lane, nb:, :])
        exchange(lane, unit, 0, True)

    def reduce(lane, unit):
        exchange_wait(unit, m_recv.at[0, unit])
        exchange_wait(unit, m_send.at[0, unit])
        mine = pl.ds(pl.multiple_of(g * nr, nr), nr)
        total = parts[lane, mine, :]
        for q in range(1, G):
            total = total + r_ref[unit, q - 1]
        m_ref[unit, mine, :] = total
        exchange(lane, unit, 1, True)

    def collect(lane, unit):
        exchange_wait(unit, m_recv.at[1, unit])
        whole = m_ref[unit]
        high, rest = split(whole)
        x_ref[lane, :nb, :LANES] = high
        x_ref[lane, :nb, LANES:] = rest
        high, rest = split(-turned(whole))
        x_ref[lane, nb:, :LANES] = high
        x_ref[lane, nb:, LANES:] = rest

    def correct(lane, unit, p):
        right = x_ref[lane]
        for block in range(0, pr, TILE):
            span = pl.ds(pl.multiple_of(p * pr + block, TILE), TILE)
            wide = pdot(psi_w[0, span, :], right) + pdot(psi_w[1, span, :], right)
            c_ref[unit, span, :] = wide[:, :LANES] + wide[:, LANES:]

    def finish(p):
        sums = []
        for u in range(U):
            unit = z * U + u
            total = c_ref[unit, piece(p), :]
            total = total + jnp.where(z > 0, s_ref[unit, piece(p), :], 0.0)
            total = total + jnp.where(z < B - 1, s_ref[B * U + u, piece(p), :], 0.0)
            sums.append(a_ref[unit, piece(p), :] - total)
        for part in range(2):
            half = slice(part * HALF, (part + 1) * HALF)
            out_ref[part, piece(p), :] = jnp.concatenate([total[:, half] for total in sums], axis=1)

    def step(n, carry):
        k, p = n // PIECES + 1, lax.rem(n, PIECES)
        for lane in range(2):
            at = place(lane)
            arrives, has, unit = gathered(lane, k)

            @pl.when(arrives)
            def _(lane=lane, at=at, unit=unit):
                a_copy(lane, unit, p).wait_recv()

                @pl.when(at < B - 1)
                def _():
                    a_copy(lane, unit, p).start()

            if U == 2:
                @pl.when((at > 0) & (at < B - 1) & (k == U * at) & (p == PIECES - 1))
                def _(lane=lane):
                    send_last(lane)

            arrives, dest, u = reduced(lane, k)

            @pl.when(arrives)
            def _(lane=lane, at=at, dest=dest, u=u):
                slot = s_slot(lane, at, dest, u)
                s_wait(slot, p)

                @pl.when(dest > at)
                def _():
                    unit = true(lane, dest) * U + u
                    s_ref[slot, piece(p), :] = s_ref[slot, piece(p), :] + c_ref[unit, piece(p), :]
                    s_copy(lane, s_ref.at[slot, piece(p)], unit, s_slot(lane, at + 1, dest, u), p).start()

        for lane in range(2):
            _, has, unit = gathered(lane, k - 1)

            @pl.when(has & (p == 0))
            def _(lane=lane, unit=unit):
                reduce(lane, unit)

            @pl.when(has & (p == 1))
            def _(lane=lane, unit=unit):
                collect(lane, unit)

            @pl.when(has & ((p == 1) | (p == 2)))
            def _(lane=lane, unit=unit):
                away = 1 - lane

                def one(i, carry):
                    c = 2 * (p - 1) + i
                    correct(lane, unit, c)

                    @pl.when((place(away) == 0) & (unit // U != z))
                    def _():
                        dest = true(away, unit // U)
                        slot = s_slot(away, 1, dest, lax.rem(unit, U))
                        s_copy(away, c_ref.at[unit, piece(c)], unit, slot, c).start()

                    return carry

                lax.fori_loop(0, PIECES // 2, one, 0)

        for lane in range(2):
            _, has, unit = gathered(lane, k)

            @pl.when(has)
            def _(lane=lane, unit=unit):
                margin(lane, unit, p)

                @pl.when(p == PIECES - 1)
                def _():
                    publish(lane, unit)

        @pl.when(k == K)
        def _():
            finish(p)

        return carry

    lax.fori_loop(0, K * PIECES, step, 0)

    def drain(n, carry):
        unit, p = n // PIECES, lax.rem(n, PIECES)
        block = unit // U

        @pl.when((block <= z) & (z < B - 1))
        def _():
            a_copy(0, unit, p).wait_send()

        @pl.when((block >= z) & (z > 0))
        def _():
            a_copy(1, unit, p).wait_send()

        @pl.when(block != z)
        def _():
            ref = s_ref.at[unit, piece(p)]
            pltpu.make_async_copy(ref, ref, s_send.at[unit, p]).wait()

        @pl.when(p == 0)
        def _():
            exchange_wait(unit, m_send.at[1, unit])

        return carry

    lax.fori_loop(0, B * U * PIECES, drain, 0)


def per_device(G, B, psi, dpsi, band_weight, panel_band, slab_offset):
    _, rows, cols = dpsi.shape
    nb = psi.shape[2]
    U = cols // HALF
    delay = 2 - U
    K = U * B + delay
    units = B * U
    weight = band_weight.reshape(-1, LANES)
    smem = pl.BlockSpec(memory_space=pltpu.SMEM)
    vmem = pl.BlockSpec(memory_space=pltpu.VMEM)
    hbm = pl.BlockSpec(memory_space=pl.ANY)
    small = [pltpu.with_memory_space_constraint(x, pltpu.HBM) for x in (slab_offset, panel_band, weight)]
    flops = 2 * 2 * 2 * (2 * nb) * rows * (2 * LANES) * units
    return pl.pallas_call(
        functools.partial(kernel, G, B, U, K, delay),
        out_shape=pltpu.VMEM(dpsi.shape, F32),
        in_specs=[smem, smem, vmem, hbm, hbm],
        out_specs=vmem,
        scratch_shapes=[
            pltpu.VMEM((2, 2 * nb, rows), BF16),
            pltpu.VMEM((2, rows, 2 * nb), BF16),
            pltpu.VMEM((units, rows, LANES), F32),
            pltpu.VMEM((units + U, rows, LANES), F32),
            pltpu.VMEM((max(units, 2 * nb // LANES), rows + TILE, LANES), F32),
            pltpu.VMEM((2, nb, LANES), F32),
            pltpu.VMEM((units, G - 1, nb // G, LANES), F32),
            pltpu.VMEM((units, nb, LANES), F32),
            pltpu.VMEM((2, 2 * nb, LANES), F32),
            pltpu.VMEM((2, 2 * nb, 2 * LANES), BF16),
            pltpu.SemaphoreType.DMA((2, 2 * nb // LANES)),
            pltpu.SemaphoreType.DMA((PIECES,)),
            pltpu.SemaphoreType.DMA((2, units, PIECES)),
            pltpu.SemaphoreType.DMA((units, PIECES)),
            pltpu.SemaphoreType.DMA((units, PIECES)),
            pltpu.SemaphoreType.DMA((units + U, PIECES)),
            pltpu.SemaphoreType.DMA((2, units)),
            pltpu.SemaphoreType.DMA((2, units)),
        ],
        compiler_params=pltpu.CompilerParams(
            collective_id=0, has_side_effects=True, vmem_limit_bytes=60000000
        ),
        cost_estimate=pl.CostEstimate(flops=flops, bytes_accessed=12 << 20, transcendentals=0),
        name="project",
    )(*small, psi, dpsi)


def solution(mesh):
    in_specs = (P(None, "ga", "ba"), P(None, "ga", "ba"), P(), P("ba"), P())
    out_specs = P(None, "ga", "ba")
    return jax.shard_map(
        functools.partial(per_device, mesh.shape["ga"], mesh.shape["ba"]),
        mesh=mesh, in_specs=in_specs, out_specs=out_specs, check_vma=False,
    )
```

```python
import functools

import jax
import jax.numpy as jnp
from jax import lax
from jax.experimental import pallas as pl
from jax.experimental.pallas import tpu as pltpu
from jax.sharding import PartitionSpec as P

MESH = pl.DeviceIdType.MESH
LANES = 128
HALF = LANES // 2
PIECES = 4
TILE = 256
BF16 = jnp.bfloat16
F32 = jnp.float32


def split(value):
    high = value.astype(BF16)
    return high, (value - high.astype(F32)).astype(BF16)


def turned(packed):
    lane = lax.broadcasted_iota(jnp.int32, packed.shape, 1)
    other = pltpu.roll(packed, HALF, axis=1)
    return jnp.where(lane < HALF, other, -other)


def pdot(left, right):
    return jnp.dot(left, right, preferred_element_type=F32)


def kernel(
    G, B, U, K, delay,
    offset_ref, panel_ref, weight_ref, psi_ref, dpsi_ref, out_ref,
    psi_t, psi_w, a_ref, s_ref, c_ref, parts, r_ref, m_ref, acc, x_ref,
    psi_sem, dpsi_sem, a_send, a_recv, s_send, s_recv, m_send, m_recv,
):
    rows, cols = dpsi_ref.shape[1:]
    nb = psi_ref.shape[2]
    tiles = nb // LANES
    pr = rows // PIECES
    nr = nb // G
    g = lax.axis_index("ga")
    z = lax.axis_index("ba")

    def psi_copies():
        for part in range(2):
            for t in range(tiles):
                i = part * tiles + t
                lanes = pl.ds(t * LANES, LANES)
                yield pltpu.make_async_copy(
                    psi_ref.at[part, :, lanes], c_ref.at[i, pl.ds(0, rows)], psi_sem.at[0, i]
                )
                yield pltpu.make_async_copy(
                    psi_ref.at[part, pl.ds(0, TILE), lanes],
                    c_ref.at[i, pl.ds(rows, TILE)],
                    psi_sem.at[1, i],
                )

    def dpsi_copy(p):
        span = pl.ds(p * pr, pr)
        return pltpu.make_async_copy(dpsi_ref.at[:, span], out_ref.at[:, span], dpsi_sem.at[p])

    for p in range(PIECES):
        dpsi_copy(p).start()

    barrier = pltpu.get_barrier_semaphore()
    for q in range(1, G):
        pl.semaphore_signal(barrier, inc=1, device_id={"ga": lax.rem(g + q, G)}, device_id_type=MESH)

    @pl.when(z > 0)
    def _():
        pl.semaphore_signal(barrier, inc=1, device_id={"ba": z - 1}, device_id_type=MESH)

    @pl.when(z < B - 1)
    def _():
        pl.semaphore_signal(barrier, inc=1, device_id={"ba": z + 1}, device_id_type=MESH)

    pl.semaphore_wait(barrier, G - 1 + jnp.where(z > 0, 1, 0) + jnp.where(z < B - 1, 1, 0))

    def place(lane):
        return z if lane == 0 else B - 1 - z

    def true(lane, index):
        return index if lane == 0 else B - 1 - index

    def piece(p):
        return pl.ds(pl.multiple_of(p * pr, pr), pr)

    def a_copy(lane, unit, p):
        return pltpu.make_async_remote_copy(
            a_ref.at[unit, piece(p)], a_ref.at[unit, piece(p)],
            a_send.at[lane, unit, p], a_recv.at[unit, p],
            device_id={"ba": true(lane, jnp.minimum(place(lane) + 1, B - 1))}, device_id_type=MESH,
        )

    def s_slot(lane, at, dest, u):
        shared = true(lane, dest) * U + u
        if lane == 0:
            return shared
        return jnp.where(dest == at, B * U + u, shared)

    def s_copy(lane, source, unit, slot, p):
        return pltpu.make_async_remote_copy(
            source, s_ref.at[slot, piece(p)], s_send.at[unit, p], s_recv.at[slot, p],
            device_id={"ba": true(lane, jnp.minimum(place(lane) + 1, B - 1))}, device_id_type=MESH,
        )

    def s_wait(slot, p):
        ref = s_ref.at[slot, piece(p)]
        pltpu.make_async_copy(ref, ref, s_recv.at[slot, p]).wait()

    def gathered(lane, k):
        at = place(lane)
        count = U * at
        arrives = (k >= 1) & (k <= count)
        if U == 2:
            index = jnp.where(k <= at, at - k, k - at - 1)
            u = jnp.where(k <= at, 0, 1)
        else:
            index, u = at - k, 0 * k
        own = (2 * at + lane < B) & (k > count) & (k <= count + U)
        index = jnp.where(own, at, index)
        u = jnp.where(own, k - count - 1, u)
        has = arrives | own
        unit = jnp.where(has, true(lane, index) * U + u, 0)
        return arrives, has, unit

    def reduced(lane, k):
        at = place(lane)
        m = k - U * at - delay
        arrives = (at > 0) & (m >= 1) & (m <= U * (B - at))
        if U == 2:
            dest = jnp.where(m <= B - at, at + m - 1, 2 * B - at - m)
            u = jnp.where(m <= B - at, 0, 1)
        else:
            dest, u = at + m - 1, 0 * k
        dest = jnp.where(arrives, dest, at)
        return arrives, dest, u

    def pack(u, p):
        span = pl.ds(p * pr, pr)
        own = slice(u * HALF, (u + 1) * HALF)
        a_ref[z * U + u, span, :] = jnp.concatenate(
            [out_ref[0, span, own], out_ref[1, span, own]], axis=1
        )

    for p in range(PIECES):
        dpsi_copy(p).wait()
        pack(0, p)
        for lane in range(2):
            @pl.when(place(lane) < B - 1)
            def _(lane=lane, p=p):
                a_copy(lane, z * U, p).start()
    for copy in psi_copies():
        copy.start()
    for u in range(1, U):
        for p in range(PIECES):
            pack(u, p)

    def send_last(lane):
        if U == 2:
            for p in range(PIECES):
                a_copy(lane, z * U + 1, p).start()

    for lane in range(2):
        @pl.when((place(lane) == 0) & (B > 1))
        def _(lane=lane):
            send_last(lane)

    def prepare(p):
        @pl.when(p == 0)
        def _():
            for copy in psi_copies():
                copy.wait()

        offset = offset_ref[g]
        for part in range(2):
            for t in range(tiles):
                i = part * tiles + t
                row = weight_ref[pl.ds(panel_ref[t], 1), :]

                def load(n, carry, i=i, row=row):
                    at = p * pr + n * TILE
                    block = c_ref[i, pl.ds(lax.rem(at - offset + rows, rows), TILE), :]
                    span = pl.ds(pl.multiple_of(at, TILE), TILE)
                    bands = slice(i * LANES, (i + 1) * LANES)
                    high, rest = split(block.T)
                    psi_t[0, bands, span] = high
                    psi_t[1, bands, span] = rest
                    high, rest = split(block * row)
                    psi_w[0, span, bands] = high
                    psi_w[1, span, bands] = rest
                    return carry

                lax.fori_loop(0, pr // TILE, load, 0)

    def margin(lane, unit, p):
        high, rest = split(a_ref[unit, piece(p), :])
        right = jnp.concatenate([high, rest], axis=1)
        for block in range(0, 2 * nb, TILE):
            bands = slice(block, block + TILE)
            wide = pdot(psi_t[0, bands, piece(p)], right) + pdot(psi_t[1, bands, piece(p)], right)
            narrow = wide[:, :LANES] + wide[:, LANES:]
            acc[lane, bands, :] = jnp.where(p == 0, 0.0, acc[lane, bands, :]) + narrow

    def exchange(lane, unit, phase, start):
        for q in range(1, G):
            peer = lax.rem(g + q, G)
            if phase == 0:
                source = parts.at[lane, pl.ds(pl.multiple_of(peer * nr, nr), nr)]
                target = r_ref.at[unit, q - 1]
            else:
                source = m_ref.at[unit, pl.ds(pl.multiple_of(g * nr, nr), nr)]
                target = source
            pltpu.make_async_remote_copy(
                source, target, m_send.at[phase, unit], m_recv.at[phase, unit],
                device_id={"ga": peer}, device_id_type=MESH,
            ).start()

    def exchange_wait(unit, sem):
        ref = r_ref.at[unit]
        pltpu.make_async_copy(ref, ref, sem).wait()

    def publish(lane, unit):
        parts[lane] = acc[lane, :nb, :] + turned(acc[lane, nb:, :])
        exchange(lane, unit, 0, True)

    def reduce(lane, unit):
        exchange_wait(unit, m_recv.at[0, unit])
        exchange_wait(unit, m_send.at[0, unit])
        mine = pl.ds(pl.multiple_of(g * nr, nr), nr)
        total = parts[lane, mine, :]
        for q in range(1, G):
            total = total + r_ref[unit, q - 1]
        m_ref[unit, mine, :] = total
        exchange(lane, unit, 1, True)

    def collect(lane, unit):
        exchange_wait(unit, m_recv.at[1, unit])
        whole = m_ref[unit]
        high, rest = split(whole)
        x_ref[lane, :nb, :LANES] = high
        x_ref[lane, :nb, LANES:] = rest
        high, rest = split(-turned(whole))
        x_ref[lane, nb:, :LANES] = high
        x_ref[lane, nb:, LANES:] = rest

    def correct(lane, unit, p):
        right = x_ref[lane]
        for block in range(0, pr, TILE):
            span = pl.ds(pl.multiple_of(p * pr + block, TILE), TILE)
            wide = pdot(psi_w[0, span, :], right) + pdot(psi_w[1, span, :], right)
            c_ref[unit, span, :] = wide[:, :LANES] + wide[:, LANES:]

    def finish(p):
        sums = []
        for u in range(U):
            unit = z * U + u
            total = c_ref[unit, piece(p), :]
            total = total + jnp.where(z > 0, s_ref[unit, piece(p), :], 0.0)
            total = total + jnp.where(z < B - 1, s_ref[B * U + u, piece(p), :], 0.0)
            sums.append(a_ref[unit, piece(p), :] - total)
        for part in range(2):
            half = slice(part * HALF, (part + 1) * HALF)
            out_ref[part, piece(p), :] = jnp.concatenate([total[:, half] for total in sums], axis=1)

    def summed(lane, k, p):
        at = place(lane)
        arrives, dest, u = reduced(lane, k)

        @pl.when(arrives)
        def _():
            slot = s_slot(lane, at, dest, u)
            s_wait(slot, p)

            @pl.when(dest > at)
            def _():
                unit = true(lane, dest) * U + u
                s_ref[slot, piece(p), :] = s_ref[slot, piece(p), :] + c_ref[unit, piece(p), :]
                s_copy(lane, s_ref.at[slot, piece(p)], unit, s_slot(lane, at + 1, dest, u), p).start()

    def step(n, carry):
        k, p = n // PIECES + 1, lax.rem(n, PIECES)
        for lane in range(2):
            at = place(lane)
            arrives, has, unit = gathered(lane, k)

            @pl.when(arrives)
            def _(lane=lane, at=at, unit=unit):
                a_copy(lane, unit, p).wait_recv()

                @pl.when(at < B - 1)
                def _():
                    a_copy(lane, unit, p).start()

            if U == 2:
                @pl.when((at > 0) & (at < B - 1) & (k == U * at) & (p == PIECES - 1))
                def _(lane=lane):
                    send_last(lane)

            summed(lane, k, p)

        @pl.when(k == 1)
        def _():
            prepare(p)

        for lane in range(2):
            _, has, unit = gathered(lane, k - 1)

            @pl.when(has & (p == 0))
            def _(lane=lane, unit=unit):
                reduce(lane, unit)

            @pl.when(has & (p == 1))
            def _(lane=lane, unit=unit):
                collect(lane, unit)

            @pl.when(has & ((p == 1) | (p == 2)))
            def _(lane=lane, unit=unit):
                away = 1 - lane

                def one(i, carry):
                    c = 2 * (p - 1) + i
                    correct(lane, unit, c)

                    @pl.when((place(away) == 0) & (unit // U != z))
                    def _():
                        dest = true(away, unit // U)
                        slot = s_slot(away, 1, dest, lax.rem(unit, U))
                        s_copy(away, c_ref.at[unit, piece(c)], unit, slot, c).start()

                    return carry

                lax.fori_loop(0, PIECES // 2, one, 0)

        for lane in range(2):
            _, has, unit = gathered(lane, k)

            @pl.when(has)
            def _(lane=lane, unit=unit):
                margin(lane, unit, p)

                @pl.when(p == PIECES - 1)
                def _():
                    publish(lane, unit)

        return carry

    lax.fori_loop(0, (K - 1) * PIECES, step, 0)

    def last(p, carry):
        for lane in range(2):
            summed(lane, K, p)
        finish(p)
        return carry

    lax.fori_loop(0, PIECES - 1, last, 0)

    def drain(n, carry):
        unit, p = n // PIECES, lax.rem(n, PIECES)
        block = unit // U

        @pl.when((block <= z) & (z < B - 1))
        def _():
            a_copy(0, unit, p).wait_send()

        @pl.when((block >= z) & (z > 0))
        def _():
            a_copy(1, unit, p).wait_send()

        @pl.when(block != z)
        def _():
            ref = s_ref.at[unit, piece(p)]
            pltpu.make_async_copy(ref, ref, s_send.at[unit, p]).wait()

        @pl.when(p == 0)
        def _():
            exchange_wait(unit, m_send.at[1, unit])

        return carry

    lax.fori_loop(0, B * U * PIECES, drain, 0)
    last(PIECES - 1, 0)


def per_device(G, B, psi, dpsi, band_weight, panel_band, slab_offset):
    _, rows, cols = dpsi.shape
    nb = psi.shape[2]
    U = cols // HALF
    delay = 2 - U
    K = U * B + 2 * delay
    units = B * U
    weight = band_weight.reshape(-1, LANES)
    smem = pl.BlockSpec(memory_space=pltpu.SMEM)
    vmem = pl.BlockSpec(memory_space=pltpu.VMEM)
    hbm = pl.BlockSpec(memory_space=pl.ANY)
    small = [pltpu.with_memory_space_constraint(x, pltpu.HBM) for x in (slab_offset, panel_band, weight)]
    flops = 2 * 2 * 2 * (2 * nb) * rows * (2 * LANES) * units
    return pl.pallas_call(
        functools.partial(kernel, G, B, U, K, delay),
        out_shape=pltpu.VMEM(dpsi.shape, F32),
        in_specs=[smem, smem, vmem, hbm, hbm],
        out_specs=vmem,
        scratch_shapes=[
            pltpu.VMEM((2, 2 * nb, rows), BF16),
            pltpu.VMEM((2, rows, 2 * nb), BF16),
            pltpu.VMEM((units, rows, LANES), F32),
            pltpu.VMEM((units + U, rows, LANES), F32),
            pltpu.VMEM((max(units, 2 * nb // LANES), rows + TILE, LANES), F32),
            pltpu.VMEM((2, nb, LANES), F32),
            pltpu.VMEM((units, G - 1, nb // G, LANES), F32),
            pltpu.VMEM((units, nb, LANES), F32),
            pltpu.VMEM((2, 2 * nb, LANES), F32),
            pltpu.VMEM((2, 2 * nb, 2 * LANES), BF16),
            pltpu.SemaphoreType.DMA((2, 2 * nb // LANES)),
            pltpu.SemaphoreType.DMA((PIECES,)),
            pltpu.SemaphoreType.DMA((2, units, PIECES)),
            pltpu.SemaphoreType.DMA((units, PIECES)),
            pltpu.SemaphoreType.DMA((units, PIECES)),
            pltpu.SemaphoreType.DMA((units + U, PIECES)),
            pltpu.SemaphoreType.DMA((2, units)),
            pltpu.SemaphoreType.DMA((2, units)),
        ],
        compiler_params=pltpu.CompilerParams(
            collective_id=0, has_side_effects=True, vmem_limit_bytes=60000000
        ),
        cost_estimate=pl.CostEstimate(flops=flops, bytes_accessed=12 << 20, transcendentals=0),
        name="project",
    )(*small, psi, dpsi)


def solution(mesh):
    in_specs = (P(None, "ga", "ba"), P(None, "ga", "ba"), P(), P("ba"), P())
    out_specs = P(None, "ga", "ba")
    return jax.shard_map(
        functools.partial(per_device, mesh.shape["ga"], mesh.shape["ba"]),
        mesh=mesh, in_specs=in_specs, out_specs=out_specs, check_vma=False,
    )
```

```python
import functools

import jax
import jax.numpy as jnp
from jax import lax
from jax.experimental import pallas as pl
from jax.experimental.pallas import tpu as pltpu
from jax.sharding import PartitionSpec as P

MESH = pl.DeviceIdType.MESH
LANES = 128
HALF = LANES // 2
PIECES = 4
TILE = 256
BF16 = jnp.bfloat16
F32 = jnp.float32


def split(value):
    high = value.astype(BF16)
    return high, (value - high.astype(F32)).astype(BF16)


def turned(packed):
    lane = lax.broadcasted_iota(jnp.int32, packed.shape, 1)
    other = pltpu.roll(packed, HALF, axis=1)
    return jnp.where(lane < HALF, other, -other)


def pdot(left, right):
    return jnp.dot(left, right, preferred_element_type=F32)


def kernel(
    G, B, U, K, delay,
    offset_ref, panel_ref, weight_ref, psi_ref, dpsi_ref, out_ref,
    psi_t, psi_w, a_ref, s_ref, c_ref, parts, r_ref, m_ref, acc, x_ref,
    psi_sem, dpsi_sem, a_send, a_recv, s_send, s_recv, m_send, m_recv,
):
    rows, cols = dpsi_ref.shape[1:]
    nb = psi_ref.shape[2]
    tiles = nb // LANES
    pr = rows // PIECES
    nr = nb // G
    g = lax.axis_index("ga")
    z = lax.axis_index("ba")

    def psi_copies():
        for part in range(2):
            for t in range(tiles):
                i = part * tiles + t
                lanes = pl.ds(t * LANES, LANES)
                yield pltpu.make_async_copy(
                    psi_ref.at[part, :, lanes], c_ref.at[i, pl.ds(0, rows)], psi_sem.at[0, i]
                )
                yield pltpu.make_async_copy(
                    psi_ref.at[part, pl.ds(0, TILE), lanes],
                    c_ref.at[i, pl.ds(rows, TILE)],
                    psi_sem.at[1, i],
                )

    def dpsi_copy(p):
        span = pl.ds(p * pr, pr)
        return pltpu.make_async_copy(dpsi_ref.at[:, span], out_ref.at[:, span], dpsi_sem.at[p])

    for p in range(PIECES):
        dpsi_copy(p).start()

    barrier = pltpu.get_barrier_semaphore()
    @pl.when(z > 0)
    def _():
        pl.semaphore_signal(barrier, inc=1, device_id={"ba": z - 1}, device_id_type=MESH)

    @pl.when(z < B - 1)
    def _():
        pl.semaphore_signal(barrier, inc=1, device_id={"ba": z + 1}, device_id_type=MESH)

    for q in range(1, G):
        pl.semaphore_signal(barrier, inc=1, device_id={"ga": lax.rem(g + q, G)}, device_id_type=MESH)

    def place(lane):
        return z if lane == 0 else B - 1 - z

    def true(lane, index):
        return index if lane == 0 else B - 1 - index

    def piece(p):
        return pl.ds(pl.multiple_of(p * pr, pr), pr)

    def a_copy(lane, unit, p):
        return pltpu.make_async_remote_copy(
            a_ref.at[unit, piece(p)], a_ref.at[unit, piece(p)],
            a_send.at[lane, unit, p], a_recv.at[unit, p],
            device_id={"ba": true(lane, jnp.minimum(place(lane) + 1, B - 1))}, device_id_type=MESH,
        )

    def s_slot(lane, at, dest, u):
        shared = true(lane, dest) * U + u
        if lane == 0:
            return shared
        return jnp.where(dest == at, B * U + u, shared)

    def s_copy(lane, source, unit, slot, p):
        return pltpu.make_async_remote_copy(
            source, s_ref.at[slot, piece(p)], s_send.at[unit, p], s_recv.at[slot, p],
            device_id={"ba": true(lane, jnp.minimum(place(lane) + 1, B - 1))}, device_id_type=MESH,
        )

    def s_wait(slot, p):
        ref = s_ref.at[slot, piece(p)]
        pltpu.make_async_copy(ref, ref, s_recv.at[slot, p]).wait()

    def gathered(lane, k):
        at = place(lane)
        count = U * at
        arrives = (k >= 1) & (k <= count)
        if U == 2:
            index = jnp.where(k <= at, at - k, k - at - 1)
            u = jnp.where(k <= at, 0, 1)
        else:
            index, u = at - k, 0 * k
        own = (2 * at + lane < B) & (k > count) & (k <= count + U)
        index = jnp.where(own, at, index)
        u = jnp.where(own, k - count - 1, u)
        has = arrives | own
        unit = jnp.where(has, true(lane, index) * U + u, 0)
        return arrives, has, unit

    def reduced(lane, k):
        at = place(lane)
        m = k - U * at - delay
        arrives = (at > 0) & (m >= 1) & (m <= U * (B - at))
        if U == 2:
            dest = jnp.where(m <= B - at, at + m - 1, 2 * B - at - m)
            u = jnp.where(m <= B - at, 0, 1)
        else:
            dest, u = at + m - 1, 0 * k
        dest = jnp.where(arrives, dest, at)
        return arrives, dest, u

    def pack(u, p):
        span = pl.ds(p * pr, pr)
        own = slice(u * HALF, (u + 1) * HALF)
        a_ref[z * U + u, span, :] = jnp.concatenate(
            [out_ref[0, span, own], out_ref[1, span, own]], axis=1
        )

    for p in range(PIECES):
        dpsi_copy(p).wait()
        pack(0, p)
        if p == 0:
            pl.semaphore_wait(barrier, G - 1 + jnp.where(z > 0, 1, 0) + jnp.where(z < B - 1, 1, 0))
        for lane in range(2):
            @pl.when(place(lane) < B - 1)
            def _(lane=lane, p=p):
                a_copy(lane, z * U, p).start()
    for copy in psi_copies():
        copy.start()
    for u in range(1, U):
        for p in range(PIECES):
            pack(u, p)

    def send_last(lane):
        if U == 2:
            for p in range(PIECES):
                a_copy(lane, z * U + 1, p).start()

    for lane in range(2):
        @pl.when((place(lane) == 0) & (B > 1))
        def _(lane=lane):
            send_last(lane)

    def prepare(p):
        @pl.when(p == 0)
        def _():
            for copy in psi_copies():
                copy.wait()

        offset = offset_ref[g]
        for part in range(2):
            for t in range(tiles):
                i = part * tiles + t
                row = weight_ref[pl.ds(panel_ref[t], 1), :]

                def load(n, carry, i=i, row=row):
                    at = p * pr + n * TILE
                    block = c_ref[i, pl.ds(lax.rem(at - offset + rows, rows), TILE), :]
                    span = pl.ds(pl.multiple_of(at, TILE), TILE)
                    bands = slice(i * LANES, (i + 1) * LANES)
                    high, rest = split(block.T)
                    psi_t[0, bands, span] = high
                    psi_t[1, bands, span] = rest
                    high, rest = split(block * row)
                    psi_w[0, span, bands] = high
                    psi_w[1, span, bands] = rest
                    return carry

                lax.fori_loop(0, pr // TILE, load, 0)

    def margin(lane, unit, p):
        high, rest = split(a_ref[unit, piece(p), :])
        right = jnp.concatenate([high, rest], axis=1)
        for block in range(0, 2 * nb, TILE):
            bands = slice(block, block + TILE)
            wide = pdot(psi_t[0, bands, piece(p)], right) + pdot(psi_t[1, bands, piece(p)], right)
            narrow = wide[:, :LANES] + wide[:, LANES:]
            acc[lane, bands, :] = jnp.where(p == 0, 0.0, acc[lane, bands, :]) + narrow

    def exchange(lane, unit, phase, start):
        for q in range(1, G):
            peer = lax.rem(g + q, G)
            if phase == 0:
                source = parts.at[lane, pl.ds(pl.multiple_of(peer * nr, nr), nr)]
                target = r_ref.at[unit, q - 1]
            else:
                source = m_ref.at[unit, pl.ds(pl.multiple_of(g * nr, nr), nr)]
                target = source
            pltpu.make_async_remote_copy(
                source, target, m_send.at[phase, unit], m_recv.at[phase, unit],
                device_id={"ga": peer}, device_id_type=MESH,
            ).start()

    def exchange_wait(unit, sem):
        ref = r_ref.at[unit]
        pltpu.make_async_copy(ref, ref, sem).wait()

    def publish(lane, unit):
        parts[lane] = acc[lane, :nb, :] + turned(acc[lane, nb:, :])
        exchange(lane, unit, 0, True)

    def reduce(lane, unit):
        exchange_wait(unit, m_recv.at[0, unit])
        exchange_wait(unit, m_send.at[0, unit])
        mine = pl.ds(pl.multiple_of(g * nr, nr), nr)
        total = parts[lane, mine, :]
        for q in range(1, G):
            total = total + r_ref[unit, q - 1]
        m_ref[unit, mine, :] = total
        exchange(lane, unit, 1, True)

    def collect(lane, unit):
        exchange_wait(unit, m_recv.at[1, unit])
        whole = m_ref[unit]
        high, rest = split(whole)
        x_ref[lane, :nb, :LANES] = high
        x_ref[lane, :nb, LANES:] = rest
        high, rest = split(-turned(whole))
        x_ref[lane, nb:, :LANES] = high
        x_ref[lane, nb:, LANES:] = rest

    def correct(lane, unit, p):
        right = x_ref[lane]
        for block in range(0, pr, TILE):
            span = pl.ds(pl.multiple_of(p * pr + block, TILE), TILE)
            wide = pdot(psi_w[0, span, :], right) + pdot(psi_w[1, span, :], right)
            c_ref[unit, span, :] = wide[:, :LANES] + wide[:, LANES:]

    def finish(p):
        sums = []
        for u in range(U):
            unit = z * U + u
            total = c_ref[unit, piece(p), :]
            total = total + jnp.where(z > 0, s_ref[unit, piece(p), :], 0.0)
            total = total + jnp.where(z < B - 1, s_ref[B * U + u, piece(p), :], 0.0)
            sums.append(a_ref[unit, piece(p), :] - total)
        for part in range(2):
            half = slice(part * HALF, (part + 1) * HALF)
            out_ref[part, piece(p), :] = jnp.concatenate([total[:, half] for total in sums], axis=1)

    def summed(lane, k, p):
        at = place(lane)
        arrives, dest, u = reduced(lane, k)

        @pl.when(arrives)
        def _():
            slot = s_slot(lane, at, dest, u)
            s_wait(slot, p)

            @pl.when(dest > at)
            def _():
                unit = true(lane, dest) * U + u
                s_ref[slot, piece(p), :] = s_ref[slot, piece(p), :] + c_ref[unit, piece(p), :]
                s_copy(lane, s_ref.at[slot, piece(p)], unit, s_slot(lane, at + 1, dest, u), p).start()

    def step(n, carry):
        k, p = n // PIECES + 1, lax.rem(n, PIECES)
        for lane in range(2):
            at = place(lane)
            arrives, has, unit = gathered(lane, k)

            @pl.when(arrives)
            def _(lane=lane, at=at, unit=unit):
                a_copy(lane, unit, p).wait_recv()

                @pl.when(at < B - 1)
                def _():
                    a_copy(lane, unit, p).start()

            if U == 2:
                @pl.when((at > 0) & (at < B - 1) & (k == U * at) & (p == PIECES - 1))
                def _(lane=lane):
                    send_last(lane)

            summed(lane, k, p)

        @pl.when(k == 1)
        def _():
            prepare(p)

        for lane in range(2):
            _, has, unit = gathered(lane, k - 1)

            @pl.when(has & (p == 0))
            def _(lane=lane, unit=unit):
                reduce(lane, unit)

            @pl.when(has & (p == 1))
            def _(lane=lane, unit=unit):
                collect(lane, unit)

            @pl.when(has & ((p == 1) | (p == 2)))
            def _(lane=lane, unit=unit):
                away = 1 - lane

                def one(i, carry):
                    c = 2 * (p - 1) + i
                    correct(lane, unit, c)

                    @pl.when((place(away) == 0) & (unit // U != z))
                    def _():
                        dest = true(away, unit // U)
                        slot = s_slot(away, 1, dest, lax.rem(unit, U))
                        s_copy(away, c_ref.at[unit, piece(c)], unit, slot, c).start()

                    return carry

                lax.fori_loop(0, PIECES // 2, one, 0)

        for lane in range(2):
            _, has, unit = gathered(lane, k)

            @pl.when(has)
            def _(lane=lane, unit=unit):
                margin(lane, unit, p)

                @pl.when(p == PIECES - 1)
                def _():
                    publish(lane, unit)

        return carry

    lax.fori_loop(0, (K - 1) * PIECES, step, 0)

    def last(p, carry):
        for lane in range(2):
            summed(lane, K, p)
        finish(p)
        return carry

    lax.fori_loop(0, PIECES - 1, last, 0)

    def drain(n, carry):
        unit, p = n // PIECES, lax.rem(n, PIECES)
        block = unit // U

        @pl.when((block <= z) & (z < B - 1))
        def _():
            a_copy(0, unit, p).wait_send()

        @pl.when((block >= z) & (z > 0))
        def _():
            a_copy(1, unit, p).wait_send()

        @pl.when(block != z)
        def _():
            ref = s_ref.at[unit, piece(p)]
            pltpu.make_async_copy(ref, ref, s_send.at[unit, p]).wait()

        @pl.when(p == 0)
        def _():
            exchange_wait(unit, m_send.at[1, unit])

        return carry

    lax.fori_loop(0, B * U * PIECES, drain, 0)
    last(PIECES - 1, 0)


def per_device(G, B, psi, dpsi, band_weight, panel_band, slab_offset):
    _, rows, cols = dpsi.shape
    nb = psi.shape[2]
    U = cols // HALF
    delay = 2 - U
    K = U * B + 2 * delay
    units = B * U
    weight = band_weight.reshape(-1, LANES)
    smem = pl.BlockSpec(memory_space=pltpu.SMEM)
    vmem = pl.BlockSpec(memory_space=pltpu.VMEM)
    hbm = pl.BlockSpec(memory_space=pl.ANY)
    small = [pltpu.with_memory_space_constraint(x, pltpu.HBM) for x in (slab_offset, panel_band, weight)]
    flops = 2 * 2 * 2 * (2 * nb) * rows * (2 * LANES) * units
    return pl.pallas_call(
        functools.partial(kernel, G, B, U, K, delay),
        out_shape=pltpu.VMEM(dpsi.shape, F32),
        in_specs=[smem, smem, vmem, hbm, hbm],
        out_specs=vmem,
        scratch_shapes=[
            pltpu.VMEM((2, 2 * nb, rows), BF16),
            pltpu.VMEM((2, rows, 2 * nb), BF16),
            pltpu.VMEM((units, rows, LANES), F32),
            pltpu.VMEM((units + U, rows, LANES), F32),
            pltpu.VMEM((max(units, 2 * nb // LANES), rows + TILE, LANES), F32),
            pltpu.VMEM((2, nb, LANES), F32),
            pltpu.VMEM((units, G - 1, nb // G, LANES), F32),
            pltpu.VMEM((units, nb, LANES), F32),
            pltpu.VMEM((2, 2 * nb, LANES), F32),
            pltpu.VMEM((2, 2 * nb, 2 * LANES), BF16),
            pltpu.SemaphoreType.DMA((2, 2 * nb // LANES)),
            pltpu.SemaphoreType.DMA((PIECES,)),
            pltpu.SemaphoreType.DMA((2, units, PIECES)),
            pltpu.SemaphoreType.DMA((units, PIECES)),
            pltpu.SemaphoreType.DMA((units, PIECES)),
            pltpu.SemaphoreType.DMA((units + U, PIECES)),
            pltpu.SemaphoreType.DMA((2, units)),
            pltpu.SemaphoreType.DMA((2, units)),
        ],
        compiler_params=pltpu.CompilerParams(
            collective_id=0, has_side_effects=True, vmem_limit_bytes=60000000
        ),
        cost_estimate=pl.CostEstimate(flops=flops, bytes_accessed=12 << 20, transcendentals=0),
        name="project",
    )(*small, psi, dpsi)


def solution(mesh):
    in_specs = (P(None, "ga", "ba"), P(None, "ga", "ba"), P(), P("ba"), P())
    out_specs = P(None, "ga", "ba")
    return jax.shard_map(
        functools.partial(per_device, mesh.shape["ga"], mesh.shape["ba"]),
        mesh=mesh, in_specs=in_specs, out_specs=out_specs, check_vma=False,
    )
```

```python
import functools

import jax
import jax.numpy as jnp
from jax import lax
from jax.experimental import pallas as pl
from jax.experimental.pallas import tpu as pltpu
from jax.sharding import PartitionSpec as P

MESH = pl.DeviceIdType.MESH
LANES = 128
HALF = LANES // 2
PIECES = 4
TILE = 256
BF16 = jnp.bfloat16
F32 = jnp.float32


def split(value):
    high = value.astype(BF16)
    return high, (value - high.astype(F32)).astype(BF16)


def turned(packed):
    lane = lax.broadcasted_iota(jnp.int32, packed.shape, 1)
    other = pltpu.roll(packed, HALF, axis=1)
    return jnp.where(lane < HALF, other, -other)


def pdot(left, right):
    return jnp.dot(left, right, preferred_element_type=F32)


def kernel(
    G, B, U, K, delay,
    offset_ref, panel_ref, weight_ref, psi_ref, dpsi_ref, out_ref,
    psi_t, psi_w, a_ref, s_ref, c_ref, parts, r_ref, m_ref, acc, x_ref,
    psi_sem, dpsi_sem, a_send, a_recv, s_send, s_recv, m_send, m_recv,
):
    rows, cols = dpsi_ref.shape[1:]
    nb = psi_ref.shape[2]
    tiles = nb // LANES
    pr = rows // PIECES
    nr = nb // G
    g = lax.axis_index("ga")
    z = lax.axis_index("ba")

    def psi_copies():
        for part in range(2):
            for t in range(tiles):
                i = part * tiles + t
                lanes = pl.ds(t * LANES, LANES)
                yield pltpu.make_async_copy(
                    psi_ref.at[part, :, lanes], c_ref.at[i, pl.ds(0, rows)], psi_sem.at[0, i]
                )
                yield pltpu.make_async_copy(
                    psi_ref.at[part, pl.ds(0, TILE), lanes],
                    c_ref.at[i, pl.ds(rows, TILE)],
                    psi_sem.at[1, i],
                )

    def dpsi_copy(p):
        span = pl.ds(p * pr, pr)
        return pltpu.make_async_copy(dpsi_ref.at[:, span], out_ref.at[:, span], dpsi_sem.at[p])

    for p in range(PIECES):
        dpsi_copy(p).start()

    barrier = pltpu.get_barrier_semaphore()
    @pl.when(z > 0)
    def _():
        pl.semaphore_signal(barrier, inc=1, device_id={"ba": z - 1}, device_id_type=MESH)

    @pl.when(z < B - 1)
    def _():
        pl.semaphore_signal(barrier, inc=1, device_id={"ba": z + 1}, device_id_type=MESH)

    for q in range(1, G):
        pl.semaphore_signal(barrier, inc=1, device_id={"ga": lax.rem(g + q, G)}, device_id_type=MESH)

    def place(lane):
        return z if lane == 0 else B - 1 - z

    def true(lane, index):
        return index if lane == 0 else B - 1 - index

    def piece(p):
        return pl.ds(pl.multiple_of(p * pr, pr), pr)

    def a_copy(lane, unit, p):
        return pltpu.make_async_remote_copy(
            a_ref.at[unit, piece(p)], a_ref.at[unit, piece(p)],
            a_send.at[lane, unit, p], a_recv.at[unit, p],
            device_id={"ba": true(lane, jnp.minimum(place(lane) + 1, B - 1))}, device_id_type=MESH,
        )

    def s_slot(lane, at, dest, u):
        shared = true(lane, dest) * U + u
        if lane == 0:
            return shared
        return jnp.where(dest == at, B * U + u, shared)

    def s_copy(lane, source, unit, slot, p):
        return pltpu.make_async_remote_copy(
            source, s_ref.at[slot, piece(p)], s_send.at[unit, p], s_recv.at[slot, p],
            device_id={"ba": true(lane, jnp.minimum(place(lane) + 1, B - 1))}, device_id_type=MESH,
        )

    def s_wait(slot, p):
        ref = s_ref.at[slot, piece(p)]
        pltpu.make_async_copy(ref, ref, s_recv.at[slot, p]).wait()

    def gathered(lane, k):
        at = place(lane)
        count = U * at
        arrives = (k >= 1) & (k <= count)
        if U == 2:
            index = jnp.where(k <= at, at - k, k - at - 1)
            u = jnp.where(k <= at, 0, 1)
        else:
            index, u = at - k, 0 * k
        own = (2 * at + lane < B) & (k > count) & (k <= count + U)
        index = jnp.where(own, at, index)
        u = jnp.where(own, k - count - 1, u)
        has = arrives | own
        unit = jnp.where(has, true(lane, index) * U + u, 0)
        return arrives, has, unit

    def reduced(lane, k):
        at = place(lane)
        m = k - U * at - delay
        arrives = (at > 0) & (m >= 1) & (m <= U * (B - at))
        if U == 2:
            dest = jnp.where(m <= B - at, at + m - 1, 2 * B - at - m)
            u = jnp.where(m <= B - at, 0, 1)
        else:
            dest, u = at + m - 1, 0 * k
        dest = jnp.where(arrives, dest, at)
        return arrives, dest, u

    def pack(u, p):
        span = pl.ds(p * pr, pr)
        own = slice(u * HALF, (u + 1) * HALF)
        a_ref[z * U + u, span, :] = jnp.concatenate(
            [out_ref[0, span, own], out_ref[1, span, own]], axis=1
        )

    for p in range(PIECES):
        dpsi_copy(p).wait()
        pack(0, p)
        if p == 0:
            pl.semaphore_wait(barrier, G - 1 + jnp.where(z > 0, 1, 0) + jnp.where(z < B - 1, 1, 0))
        for lane in range(2):
            @pl.when(place(lane) < B - 1)
            def _(lane=lane, p=p):
                a_copy(lane, z * U, p).start()
    for copy in psi_copies():
        copy.start()
    for u in range(1, U):
        for p in range(PIECES):
            pack(u, p)

    def send_last(lane):
        if U == 2:
            for p in range(PIECES):
                a_copy(lane, z * U + 1, p).start()

    for lane in range(2):
        @pl.when((place(lane) == 0) & (B > 1))
        def _(lane=lane):
            send_last(lane)

    def prepare(p):
        @pl.when(p == 0)
        def _():
            for copy in psi_copies():
                copy.wait()

        offset = offset_ref[g]
        for part in range(2):
            for t in range(tiles):
                i = part * tiles + t
                row = weight_ref[pl.ds(panel_ref[t], 1), :]

                def load(n, carry, i=i, row=row):
                    at = p * pr + n * TILE
                    block = c_ref[i, pl.ds(lax.rem(at - offset + rows, rows), TILE), :]
                    span = pl.ds(pl.multiple_of(at, TILE), TILE)
                    bands = slice(i * LANES, (i + 1) * LANES)
                    high, rest = split(block.T)
                    psi_t[0, bands, span] = high
                    psi_t[1, bands, span] = rest
                    high, rest = split(block * row)
                    psi_w[0, span, bands] = high
                    psi_w[1, span, bands] = rest
                    return carry

                lax.fori_loop(0, pr // TILE, load, 0)

    def margin(lane, unit, p):
        high, rest = split(a_ref[unit, piece(p), :])
        right = jnp.concatenate([high, rest], axis=1)
        for block in range(0, 2 * nb, TILE):
            bands = slice(block, block + TILE)
            wide = pdot(psi_t[0, bands, piece(p)], right) + pdot(psi_t[1, bands, piece(p)], right)
            narrow = wide[:, :LANES] + wide[:, LANES:]
            acc[lane, bands, :] = jnp.where(p == 0, 0.0, acc[lane, bands, :]) + narrow

    def exchange(lane, unit, phase, start):
        for q in range(1, G):
            peer = lax.rem(g + q, G)
            if phase == 0:
                source = parts.at[lane, pl.ds(pl.multiple_of(peer * nr, nr), nr)]
                target = r_ref.at[unit, q - 1]
            else:
                source = m_ref.at[unit, pl.ds(pl.multiple_of(g * nr, nr), nr)]
                target = source
            pltpu.make_async_remote_copy(
                source, target, m_send.at[phase, unit], m_recv.at[phase, unit],
                device_id={"ga": peer}, device_id_type=MESH,
            ).start()

    def exchange_wait(unit, sem):
        ref = r_ref.at[unit]
        pltpu.make_async_copy(ref, ref, sem).wait()

    def publish(lane, unit):
        parts[lane] = acc[lane, :nb, :] + turned(acc[lane, nb:, :])
        exchange(lane, unit, 0, True)

    def reduce(lane, unit):
        exchange_wait(unit, m_recv.at[0, unit])
        exchange_wait(unit, m_send.at[0, unit])
        mine = pl.ds(pl.multiple_of(g * nr, nr), nr)
        total = parts[lane, mine, :]
        for q in range(1, G):
            total = total + r_ref[unit, q - 1]
        m_ref[unit, mine, :] = total
        exchange(lane, unit, 1, True)

    def collect(lane, unit):
        exchange_wait(unit, m_recv.at[1, unit])
        whole = m_ref[unit]
        high, rest = split(whole)
        x_ref[lane, :nb, :LANES] = high
        x_ref[lane, :nb, LANES:] = rest
        high, rest = split(-turned(whole))
        x_ref[lane, nb:, :LANES] = high
        x_ref[lane, nb:, LANES:] = rest

    def correct(lane, unit, p):
        right = x_ref[lane]
        for block in range(0, pr, TILE):
            span = pl.ds(pl.multiple_of(p * pr + block, TILE), TILE)
            wide = pdot(psi_w[0, span, :], right) + pdot(psi_w[1, span, :], right)
            c_ref[unit, span, :] = wide[:, :LANES] + wide[:, LANES:]

    def arrived(u, p):
        lower = jnp.where(z > 0, s_ref[z * U + u, piece(p), :], 0.0)
        return lower + jnp.where(z < B - 1, s_ref[B * U + u, piece(p), :], 0.0)

    def settle(p, carry):
        for u in range(U):
            unit = z * U + u
            kept = a_ref[unit, piece(p), :] - c_ref[unit, piece(p), :]
            c_ref[unit, piece(p), :] = kept - arrived(u, p) if u < 1 else kept
        return carry

    def finish(p):
        sums = [c_ref[z * U + u, piece(p), :] for u in range(U)]
        if U == 2:
            sums[1] = sums[1] - arrived(1, p)
        for part in range(2):
            half = slice(part * HALF, (part + 1) * HALF)
            out_ref[part, piece(p), :] = jnp.concatenate([total[:, half] for total in sums], axis=1)

    def summed(lane, k, p):
        at = place(lane)
        arrives, dest, u = reduced(lane, k)

        @pl.when(arrives)
        def _():
            slot = s_slot(lane, at, dest, u)
            s_wait(slot, p)

            @pl.when(dest > at)
            def _():
                unit = true(lane, dest) * U + u
                s_ref[slot, piece(p), :] = s_ref[slot, piece(p), :] + c_ref[unit, piece(p), :]
                s_copy(lane, s_ref.at[slot, piece(p)], unit, s_slot(lane, at + 1, dest, u), p).start()

    def step(n, carry):
        k, p = n // PIECES + 1, lax.rem(n, PIECES)
        for lane in range(2):
            at = place(lane)
            arrives, has, unit = gathered(lane, k)

            @pl.when(arrives)
            def _(lane=lane, at=at, unit=unit):
                a_copy(lane, unit, p).wait_recv()

                @pl.when(at < B - 1)
                def _():
                    a_copy(lane, unit, p).start()

            if U == 2:
                @pl.when((at > 0) & (at < B - 1) & (k == U * at) & (p == PIECES - 1))
                def _(lane=lane):
                    send_last(lane)

            summed(lane, k, p)

        @pl.when(k == 1)
        def _():
            prepare(p)

        for lane in range(2):
            _, has, unit = gathered(lane, k - 1)

            @pl.when(has & (p == 0))
            def _(lane=lane, unit=unit):
                reduce(lane, unit)

            @pl.when(has & (p == 1))
            def _(lane=lane, unit=unit):
                collect(lane, unit)

            @pl.when(has & ((p == 1) | (p == 2)))
            def _(lane=lane, unit=unit):
                away = 1 - lane

                def one(i, carry):
                    c = 2 * (p - 1) + i
                    correct(lane, unit, c)

                    @pl.when((place(away) == 0) & (unit // U != z))
                    def _():
                        dest = true(away, unit // U)
                        slot = s_slot(away, 1, dest, lax.rem(unit, U))
                        s_copy(away, c_ref.at[unit, piece(c)], unit, slot, c).start()

                    return carry

                lax.fori_loop(0, PIECES // 2, one, 0)

        for lane in range(2):
            _, has, unit = gathered(lane, k)

            @pl.when(has)
            def _(lane=lane, unit=unit):
                margin(lane, unit, p)

                @pl.when(p == PIECES - 1)
                def _():
                    publish(lane, unit)

        return carry

    lax.fori_loop(0, (K - 1) * PIECES, step, 0)
    lax.fori_loop(0, PIECES, settle, 0)

    def last(p, carry):
        for lane in range(2):
            summed(lane, K, p)
        finish(p)
        return carry

    lax.fori_loop(0, PIECES - 1, last, 0)

    def drain(n, carry):
        unit, p = n // PIECES, lax.rem(n, PIECES)
        block = unit // U

        @pl.when((block <= z) & (z < B - 1))
        def _():
            a_copy(0, unit, p).wait_send()

        @pl.when((block >= z) & (z > 0))
        def _():
            a_copy(1, unit, p).wait_send()

        @pl.when(block != z)
        def _():
            ref = s_ref.at[unit, piece(p)]
            pltpu.make_async_copy(ref, ref, s_send.at[unit, p]).wait()

        @pl.when(p == 0)
        def _():
            exchange_wait(unit, m_send.at[1, unit])

        return carry

    lax.fori_loop(0, B * U * PIECES, drain, 0)
    last(PIECES - 1, 0)


def per_device(G, B, psi, dpsi, band_weight, panel_band, slab_offset):
    _, rows, cols = dpsi.shape
    nb = psi.shape[2]
    U = cols // HALF
    delay = 2 - U
    K = U * B + 2 * delay
    units = B * U
    weight = band_weight.reshape(-1, LANES)
    smem = pl.BlockSpec(memory_space=pltpu.SMEM)
    vmem = pl.BlockSpec(memory_space=pltpu.VMEM)
    hbm = pl.BlockSpec(memory_space=pl.ANY)
    small = [pltpu.with_memory_space_constraint(x, pltpu.HBM) for x in (slab_offset, panel_band, weight)]
    flops = 2 * 2 * 2 * (2 * nb) * rows * (2 * LANES) * units
    return pl.pallas_call(
        functools.partial(kernel, G, B, U, K, delay),
        out_shape=pltpu.VMEM(dpsi.shape, F32),
        in_specs=[smem, smem, vmem, hbm, hbm],
        out_specs=vmem,
        scratch_shapes=[
            pltpu.VMEM((2, 2 * nb, rows), BF16),
            pltpu.VMEM((2, rows, 2 * nb), BF16),
            pltpu.VMEM((units, rows, LANES), F32),
            pltpu.VMEM((units + U, rows, LANES), F32),
            pltpu.VMEM((max(units, 2 * nb // LANES), rows + TILE, LANES), F32),
            pltpu.VMEM((2, nb, LANES), F32),
            pltpu.VMEM((units, G - 1, nb // G, LANES), F32),
            pltpu.VMEM((units, nb, LANES), F32),
            pltpu.VMEM((2, 2 * nb, LANES), F32),
            pltpu.VMEM((2, 2 * nb, 2 * LANES), BF16),
            pltpu.SemaphoreType.DMA((2, 2 * nb // LANES)),
            pltpu.SemaphoreType.DMA((PIECES,)),
            pltpu.SemaphoreType.DMA((2, units, PIECES)),
            pltpu.SemaphoreType.DMA((units, PIECES)),
            pltpu.SemaphoreType.DMA((units, PIECES)),
            pltpu.SemaphoreType.DMA((units + U, PIECES)),
            pltpu.SemaphoreType.DMA((2, units)),
            pltpu.SemaphoreType.DMA((2, units)),
        ],
        compiler_params=pltpu.CompilerParams(
            collective_id=0, has_side_effects=True, vmem_limit_bytes=60000000
        ),
        cost_estimate=pl.CostEstimate(flops=flops, bytes_accessed=12 << 20, transcendentals=0),
        name="project",
    )(*small, psi, dpsi)


def solution(mesh):
    in_specs = (P(None, "ga", "ba"), P(None, "ga", "ba"), P(), P("ba"), P())
    out_specs = P(None, "ga", "ba")
    return jax.shard_map(
        functools.partial(per_device, mesh.shape["ga"], mesh.shape["ba"]),
        mesh=mesh, in_specs=in_specs, out_specs=out_specs, check_vma=False,
    )
```
